32 devices in a mesh: kgrp: 8 (over z, x), scr: 4 (over y, core).
Axes of the slice: x: 2, y: 2, z: 4, core: 2. Of those that a mesh axis runs over, the one named last changes fastest.
Arguments:
- wave_val: bfloat16 [8, 32, 2048], P('kgrp', None, 'scr'), may hold values from -6 to 6
- wave_con: bfloat16 [8, 32, 2048], P('kgrp', None, 'scr'), may hold values from -6 to 6
- excite: bfloat16 [8, 1024, 16], P('kgrp', 'scr'), may hold values from -6 to 6
- screening: bfloat16 [8, 2048, 2048], P('kgrp', None, 'scr'), may hold values from -9.1552734e-05 to 9.1552734e-05
- pair_count: int32 [8], P('kgrp'), may hold values from 1 to 2, as said below
- pair_kpoint: int32 [8, 2], P('kgrp'), may hold values from 0 to 7
- pair_partner: int32 [8, 2], P('kgrp'), may hold values from 0 to 7
Outputs:
- forward: float32 [8, 2, 1024, 16], P('kgrp', None, 'scr')
- transposed: float32 [8, 2, 1024, 16], P('kgrp', None, 'scr')
The draws below stay inside these ranges and needn't reach their ends.
Inputs may be any that keep to these rules, and one draw needn't show every extreme that they name: Slot p of screening owner h is live when p < pair_count[h]; in every draw some owner has 2 live slots.
All inputs are finite; a program needn't handle non-finite values.
Results may differ from the reference program's by a relative error of at most 0.0057.
Values may be sent and summed in bfloat16 or wider, within the bound.
No kernel may reach another device: no remote copies, remote signals or barrier semaphores. Data moves between devices by JAX's collectives and lax.ppermute only.
A program may use at most 128 MiB of HBM per device.

```python
import jax
import jax.numpy as jnp
from jax import lax

NV = 32
NC = 32
NMU = 2048
PTS_BLK = 128
MAXP = 2
NEXC = 16
NPB = 1024
NK = 8
NQ = 8


def draw_pair_count(key, part):
    first_key, second_key = jax.random.split(jax.random.fold_in(key, 17))
    counts = jax.random.randint(first_key, (NQ,), 1, MAXP + 1)
    place = jax.random.randint(second_key, (), 0, NQ)
    return jnp.where(jnp.arange(NQ) == place, MAXP, counts).astype(jnp.int32)


def place_ends(entries, stream_key, least, top_value):
    spot = [jax.random.randint(jax.random.fold_in(stream_key, axis), (), 0, length) for axis, length in enumerate(entries.shape)]
    longest = entries.shape.index(max(entries.shape))
    beside = spot[:longest] + [(spot[longest] + 1) % entries.shape[longest]] + spot[longest + 1:]
    return entries.at[tuple(spot)].set(least).at[tuple(beside)].set(top_value)


def levels(key, dims, shards, least, largest):
    gain = 1.0
    for axis_at, blocks in shards:
        heights = jax.random.uniform(jax.random.fold_in(jax.random.fold_in(key, 6), axis_at), (blocks,), jnp.float32, least / len(shards), largest / len(shards))
        gain = gain * jnp.repeat(jnp.exp(heights), dims[axis_at] // blocks).reshape((-1,) + (1,) * (len(dims) - 1 - axis_at))
    return gain


def noise(key, shape, deviation, limit, pieces=(), kind=jnp.bfloat16):
    entries = deviation * jax.random.normal(key, shape, jnp.float32)
    if pieces:
        entries = entries * levels(key, shape, pieces, -0.22, 0.18)
    return jnp.clip(entries, -limit, limit).astype(kind)


def setup_inputs(seed: int = 0) -> dict:
    streams_of = jax.random.split(jax.random.key(seed), 8)
    wave_val = noise(streams_of[0], (NK, NV, NMU), 1.0, 6.0, ((0, 8), (2, 4)))
    wave_con = noise(streams_of[1], (NK, NC, NMU), 1.0, 6.0, ((0, 8), (2, 4)))
    excite = noise(streams_of[2], (NK, NPB, NEXC), 1.0, 6.0, ((0, 8), (1, 4)))
    screening = noise(streams_of[3], (NQ, NMU, NMU), (NV * NC * NMU * NMU) ** -0.5, 9.1552734375e-05, ((0, 8), (2, 4)))
    pair_count = draw_pair_count(jax.random.fold_in(streams_of[7], 71), 0)
    pair_kpoint = place_ends(jax.random.randint(streams_of[5], (NQ, MAXP), 0, NK), jax.random.fold_in(streams_of[5], 1), 0, NK - 1).astype(jnp.int32)
    pair_partner = place_ends(jax.random.randint(streams_of[6], (NQ, MAXP), 0, NK), jax.random.fold_in(streams_of[6], 1), 0, NK - 1).astype(jnp.int32)
    return dict(wave_val=wave_val, wave_con=wave_con, excite=excite, screening=screening, pair_count=pair_count, pair_kpoint=pair_kpoint, pair_partner=pair_partner)


def pair_terms(indices, wave_val, wave_con, excite, screening):
    owner = indices[0]
    first = indices[1]
    second = indices[2]
    weights = lax.dynamic_index_in_dim(screening, owner, 0, keepdims=False)
    val_first = lax.dynamic_index_in_dim(wave_val, first, 0, keepdims=False).astype(jnp.float32)
    val_second = lax.dynamic_index_in_dim(wave_val, second, 0, keepdims=False).astype(jnp.float32)
    con_first = lax.dynamic_index_in_dim(wave_con, first, 0, keepdims=False).astype(jnp.float32)
    con_second = lax.dynamic_index_in_dim(wave_con, second, 0, keepdims=False).astype(jnp.float32)
    exc_first = lax.dynamic_index_in_dim(excite, first, 0, keepdims=False).astype(jnp.float32).reshape(NV, NC, NEXC)
    exc_second = lax.dynamic_index_in_dim(excite, second, 0, keepdims=False).astype(jnp.float32).reshape(NV, NC, NEXC)
    rho_con = (con_first[:, None, :] * con_second[None, :, :]).astype(jnp.bfloat16).reshape(NC * NC, NMU)
    screened = jnp.dot(rho_con, weights, preferred_element_type=jnp.float32).astype(jnp.bfloat16)
    rho_val = (val_first.T[:, :, None] * val_second.T[:, None, :]).astype(jnp.bfloat16).reshape(NMU, NV * NV)

    def add_block(carried, block_index):
        offset = (block_index * PTS_BLK).astype(jnp.int32)
        part_screen = lax.dynamic_slice_in_dim(screened, offset, PTS_BLK, 1)
        part_val = lax.dynamic_slice_in_dim(rho_val, offset, PTS_BLK, 0)
        kernel = jnp.dot(part_screen, part_val, preferred_element_type=jnp.float32).astype(jnp.bfloat16)
        kernel = lax.optimization_barrier(kernel).astype(jnp.float32).reshape(NC, NC, NV, NV)
        ahead = carried[0] + jnp.einsum("cdvw,wde->vce", kernel, exc_second, precision=lax.Precision.HIGHEST)
        back = carried[1] + jnp.einsum("cdvw,vce->wde", kernel, exc_first, precision=lax.Precision.HIGHEST)
        return (ahead, back), None

    zeros = jnp.zeros((NV, NC, NEXC), jnp.float32)
    totals, unused = lax.scan(add_block, (zeros, zeros), jnp.arange(NMU // PTS_BLK, dtype=jnp.int32))
    return totals[0].reshape(NPB, NEXC), totals[1].reshape(NPB, NEXC)


def reference(wave_val, wave_con, excite, screening, pair_count, pair_kpoint, pair_partner):
    owners = jnp.repeat(jnp.arange(NQ, dtype=jnp.int32), MAXP)
    indices = jnp.stack([owners, pair_kpoint.reshape(-1).astype(jnp.int32), pair_partner.reshape(-1).astype(jnp.int32)], axis=1)
    ahead, back = lax.map(lambda row: pair_terms(row, wave_val, wave_con, excite, screening), indices)
    live = (jnp.arange(MAXP, dtype=jnp.int32)[None, :] < pair_count[:, None]).astype(jnp.float32)
    live = live[:, :, None, None]
    forward = ahead.reshape(NQ, MAXP, NPB, NEXC) * live
    transposed = back.reshape(NQ, MAXP, NPB, NEXC) * live
    return forward, transposed
```

```python
import functools

import jax
import jax.numpy as jnp
from jax import lax
from jax.experimental import pallas as pl
from jax.experimental.pallas import tpu as pltpu
from jax.sharding import PartitionSpec as P

LANES = 128
F32 = jnp.float32
BF16 = jnp.bfloat16


def pick_kernel(rows, roles_ref, all_ref, out_ref):
    for i in range(out_ref.shape[0]):
        out_ref[i] = all_ref[roles_ref[i], :rows, :]


def nt(a, b):
    return lax.dot_general(a, b, (((1,), (1,)), ((), ())), preferred_element_type=F32)


def pair_products(outer, inner, out_ref, column):
    width = inner.shape[1]
    count = inner.shape[0]
    for i in range(outer.shape[0]):
        out_ref[i * count : (i + 1) * count, column : column + width] = (
            outer[i : i + 1, :] * inner
        ).astype(BF16)


def spread_blocks(kernel, out_ref, group):
    block = kernel.shape[0] // group
    tile = out_ref.shape[1] // group
    for i in range(group):
        for q in range(kernel.shape[1] // tile):
            out_ref[q * block : (q + 1) * block, i * tile : (i + 1) * tile] = kernel[
                i * block : (i + 1) * block, q * tile : (q + 1) * tile
            ]


def main_kernel(
    sizes, roles_ref, gath_ref, all_ref, weights_ref, out_ref,
    rho_ref, vals_ref, screened_ref, spread_ref, vec_ref, diag_ref,
):
    slots, nval, ncon, nexc = sizes
    shards = gath_ref.shape[0]
    mu_dev = weights_ref.shape[1]
    rows_dev = nval * ncon // shards
    exc_rows = nexc * rows_dev // mu_dev
    per = LANES // nexc
    val_at = ncon + exc_rows
    lane = lax.broadcasted_iota(jnp.int32, (per * nval, LANES), 1)
    row = lax.broadcasted_iota(jnp.int32, (per * nval, LANES), 0)
    mask = (row // nval == lane // nexc).astype(BF16)
    e_row = lax.broadcasted_iota(jnp.int32, (nexc, LANES), 0)
    e_lane = lax.broadcasted_iota(jnp.int32, (nexc, LANES), 1)
    repeat = (e_lane % nexc == e_row).astype(BF16)
    for p in range(slots):
        for s in range(shards):
            pair_products(
                gath_ref[s, slots + p, :ncon, :].astype(F32),
                gath_ref[s, p, :ncon, :].astype(F32),
                rho_ref, s * mu_dev,
            )
        screened_ref[...] = jnp.dot(
            rho_ref[...], weights_ref[...], preferred_element_type=F32
        ).astype(BF16)
        pair_products(
            all_ref[roles_ref[p], val_at : val_at + nval, :].astype(F32),
            all_ref[roles_ref[slots + p], val_at : val_at + nval, :].astype(F32),
            vals_ref, 0,
        )
        for way in range(2):
            who = slots + p if way == 0 else p
            for s in range(shards):
                part = gath_ref[s, who, ncon:val_at, :]
                flip = jnp.concatenate(
                    [part[:, i * rows_dev : (i + 1) * rows_dev] for i in range(mu_dev // rows_dev)], axis=0
                )
                vec_ref[s * rows_dev : (s + 1) * rows_dev, :] = lax.dot_general(
                    flip, repeat, (((0,), (0,)), ((), ())), preferred_element_type=F32
                )
            if way == 0:
                kernel = nt(screened_ref[...], vals_ref[...]).astype(BF16)
                count, length = ncon, nval
            else:
                kernel = nt(vals_ref[...], screened_ref[...]).astype(BF16)
                count, length = nval, ncon
            spread_blocks(kernel, spread_ref, count)
            for i in range(count):
                if way == 0:
                    vec = vec_ref[pl.ds(i, length, stride=count), :]
                else:
                    vec = vec_ref[i * length : (i + 1) * length, :]
                vec = vec.astype(BF16)
                tile = per * length
                diag_ref[i * tile : (i + 1) * tile, :] = (
                    jnp.concatenate([vec] * per, axis=0) * mask
                )
            total = jnp.dot(spread_ref[...], diag_ref[...], preferred_element_type=F32).astype(BF16)
            parts = out_ref.shape[0]
            if way == 0:
                for s in range(parts):
                    out_ref[s, p, way] = total[s * ncon : (s + 1) * ncon, :]
            else:
                total = total.reshape(ncon // per, parts, nval // parts, LANES)
                for s in range(parts):
                    out_ref[s, p, way] = total[:, s].reshape(ncon, LANES)


def body(wave_val, wave_con, excite, screening, pair_count, pair_kpoint, pair_partner):
    groups = lax.axis_size("kgrp")
    shards = lax.axis_size("scr")
    slots = pair_kpoint.shape[1]
    nval, mu_dev = wave_val.shape[1:]
    ncon = wave_con.shape[1]
    rows_dev, nexc = excite.shape[1:]
    roles = jnp.concatenate([pair_kpoint[0], pair_partner[0]])
    flip = excite[0].T
    step = mu_dev // rows_dev
    exc_rows = nexc // step
    packed = jnp.concatenate(
        [flip[i * exc_rows : (i + 1) * exc_rows] for i in range(step)], axis=1
    )
    mine = jnp.concatenate([wave_con[0], packed, wave_val[0]], axis=0)
    everyone = lax.all_to_all(
        jnp.broadcast_to(mine[None], (groups,) + mine.shape), "kgrp", 0, 0, tiled=True
    )
    keep = ncon + exc_rows
    vmem = pl.BlockSpec(memory_space=pltpu.VMEM)
    smem = pl.BlockSpec(memory_space=pltpu.SMEM)
    selected = pl.pallas_call(
        functools.partial(pick_kernel, keep),
        out_shape=jax.ShapeDtypeStruct((2 * slots, keep, mu_dev), BF16),
        in_specs=[smem, vmem],
        out_specs=vmem,
    )(roles, everyone)
    gathered = lax.all_gather(selected, "scr", axis=0, tiled=False)
    npb = nval * ncon
    per = LANES // nexc
    parts = nval // per
    split = shards // parts
    partial = pl.pallas_call(
        functools.partial(main_kernel, (slots, nval, ncon, nexc)),
        out_shape=jax.ShapeDtypeStruct((parts, slots, 2, ncon, LANES), BF16),
        in_specs=[smem, vmem, vmem, vmem],
        out_specs=vmem,
        scratch_shapes=[
            pltpu.VMEM((npb, shards * mu_dev), BF16),
            pltpu.VMEM((npb, mu_dev), BF16),
            pltpu.VMEM((npb, mu_dev), BF16),
            pltpu.VMEM((npb // per, npb * per), BF16),
            pltpu.VMEM((npb, LANES), F32),
            pltpu.VMEM((npb * per, LANES), BF16),
        ],
        compiler_params=pltpu.CompilerParams(vmem_limit_bytes=48 * 2**20),
    )(roles, gathered, everyone, screening[0])
    ahead = partial[:, :, 0].reshape(parts, slots, ncon, split, per // split, nexc)
    ahead = ahead.transpose(0, 3, 1, 2, 4, 5).reshape(shards, slots, -1)
    back = partial[:, :, 1].reshape(parts, slots, ncon // per, split, per // split, LANES)
    back = back.transpose(0, 3, 1, 2, 4, 5).reshape(shards, slots, -1)
    if split == 1:
        sent = partial
    else:
        sent = jnp.stack([ahead, back], axis=2)
    taken = lax.all_to_all(sent, "scr", 0, 0, tiled=True)
    summed = jnp.sum(taken.astype(F32), axis=0)
    live = (jnp.arange(slots, dtype=jnp.int32) < pair_count[0]).astype(F32)
    summed = summed * live.reshape((slots,) + (1,) * (summed.ndim - 1))
    few = per // split
    ahead = summed[:, 0].reshape(slots, ncon, few, nexc).transpose(0, 2, 1, 3)
    back = summed[:, 1].reshape(slots, ncon // per, few, per, nexc).transpose(0, 2, 1, 3, 4)
    shape = (1, slots, rows_dev, nexc)
    return ahead.reshape(shape), back.reshape(shape)


def solution(mesh):
    return jax.shard_map(
        body,
        mesh=mesh,
        in_specs=(
            P("kgrp", None, "scr"),
            P("kgrp", None, "scr"),
            P("kgrp", "scr", None),
            P("kgrp", None, "scr"),
            P("kgrp"),
            P("kgrp", None),
            P("kgrp", None),
        ),
        out_specs=(P("kgrp", None, "scr", None), P("kgrp", None, "scr", None)),
        check_vma=False,
    )
```

```python
import functools

import jax
import jax.numpy as jnp
from jax import lax
from jax.experimental import pallas as pl
from jax.experimental.pallas import tpu as pltpu
from jax.sharding import PartitionSpec as P

LANES = 128
F32 = jnp.float32
BF16 = jnp.bfloat16


def prepare_kernel(con_ref, exc_ref, val_ref, first_ref, second_ref):
    ncon = con_ref.shape[1]
    rows_dev = exc_ref.shape[1]
    step = con_ref.shape[2] // rows_dev
    exc_rows = exc_ref.shape[0] // step
    packed = jnp.concatenate(
        [exc_ref[i * exc_rows : (i + 1) * exc_rows, :] for i in range(step)], axis=1
    )
    for k in range(first_ref.shape[0]):
        first_ref[k, :ncon, :] = con_ref[0]
        first_ref[k, ncon:, :] = packed
        second_ref[k] = val_ref[0]


def pick_kernel(a_ref, b_ref, all_ref, out_ref):
    slots = a_ref.shape[1]
    for p in range(slots):
        out_ref[p] = all_ref[a_ref[0, p]]
        out_ref[slots + p] = all_ref[b_ref[0, p]]


def nt(a, b):
    return lax.dot_general(a, b, (((1,), (1,)), ((), ())), preferred_element_type=F32)


def pair_products(outer, inner, out_ref, column):
    width = inner.shape[1]
    count = inner.shape[0]
    for i in range(outer.shape[0]):
        out_ref[i * count : (i + 1) * count, column : column + width] = (
            outer[i : i + 1, :] * inner
        ).astype(BF16)


def spread_blocks(kernel, out_ref, group):
    block = kernel.shape[0] // group
    tile = out_ref.shape[1] // group
    for i in range(group):
        for q in range(kernel.shape[1] // tile):
            out_ref[q * block : (q + 1) * block, i * tile : (i + 1) * tile] = kernel[
                i * block : (i + 1) * block, q * tile : (q + 1) * tile
            ]


def lay_out(total, parts, nexc):
    flip = total.T
    inner = total.shape[0] // parts
    rows = []
    for s in range(parts):
        rows.append(
            jnp.concatenate(
                [
                    flip[i * nexc : (i + 1) * nexc, s * inner : (s + 1) * inner]
                    for i in range(total.shape[1] // nexc)
                ],
                axis=1,
            )
        )
    return jnp.concatenate(rows, axis=0)


def main_kernel(
    sizes, a_ref, b_ref, me_ref, gath_ref, all_ref, weights_ref, *rest
):
    *out_refs, done_ref, rho_ref, vals_ref, screened_ref, spread_ref, vec_ref, diag_ref = rest
    slots, nval, ncon, nexc = sizes
    shards = gath_ref.shape[0]
    mu_dev = weights_ref.shape[1]
    rows_dev = nval * ncon // shards
    per = LANES // nexc
    parts = done_ref.shape[0]
    lane = lax.broadcasted_iota(jnp.int32, (per * nval, LANES), 1)
    row = lax.broadcasted_iota(jnp.int32, (per * nval, LANES), 0)
    mask = (row // nval == lane // nexc).astype(BF16)
    e_row = lax.broadcasted_iota(jnp.int32, (nexc, LANES), 0)
    e_lane = lax.broadcasted_iota(jnp.int32, (nexc, LANES), 1)
    repeat = (e_lane % nexc == e_row).astype(BF16)
    wide = ncon * per
    src = lax.broadcasted_iota(jnp.int32, (wide, wide), 0)
    dst = lax.broadcasted_iota(jnp.int32, (wide, wide), 1)
    few = nval // parts
    outer = ncon // per
    moved = (src % few) * ncon + (src // few) % outer * per + src // (few * outer)
    order = (moved == dst).astype(BF16)
    for p in range(slots):
        for s in range(shards):
            pair_products(
                gath_ref[s, slots + p, :ncon, :].astype(F32),
                gath_ref[s, p, :ncon, :].astype(F32),
                rho_ref, s * mu_dev,
            )
        screened_ref[...] = jnp.dot(
            rho_ref[...], weights_ref[...], preferred_element_type=F32
        ).astype(BF16)
        pair_products(
            all_ref[a_ref[0, p]].astype(F32), all_ref[b_ref[0, p]].astype(F32), vals_ref, 0
        )
        for way in range(2):
            who = slots + p if way == 0 else p
            for s in range(shards):
                part = gath_ref[s, who, ncon:, :]
                flip = jnp.concatenate(
                    [part[:, i * rows_dev : (i + 1) * rows_dev] for i in range(mu_dev // rows_dev)], axis=0
                )
                vec_ref[s * rows_dev : (s + 1) * rows_dev, :] = lax.dot_general(
                    flip, repeat, (((0,), (0,)), ((), ())), preferred_element_type=F32
                )
            if way == 0:
                kernel = nt(screened_ref[...], vals_ref[...]).astype(BF16)
                count, length = ncon, nval
            else:
                kernel = nt(vals_ref[...], screened_ref[...]).astype(BF16)
                count, length = nval, ncon
            spread_blocks(kernel, spread_ref, count)
            for i in range(count):
                if way == 0:
                    vec = vec_ref[pl.ds(i, length, stride=count), :]
                else:
                    vec = vec_ref[i * length : (i + 1) * length, :]
                vec = vec.astype(BF16)
                tile = per * length
                diag_ref[i * tile : (i + 1) * tile, :] = (
                    jnp.concatenate([vec] * per, axis=0) * mask
                )
            total = jnp.dot(spread_ref[...], diag_ref[...], preferred_element_type=F32)
            if way == 0:
                done = lay_out(total, parts, nexc)
            else:
                total = total.reshape(outer, parts, few, LANES)
                total = jnp.concatenate(
                    [total[q, s] for s in range(parts) for q in range(outer)], axis=0
                )
                done = jnp.dot(
                    lay_out(total, parts, nexc).astype(BF16), order, preferred_element_type=F32
                )
            done = done.astype(BF16)
            for s in range(parts):
                done_ref[s, p, way] = done[s * nexc : (s + 1) * nexc, :]
    for m, out_ref in enumerate(out_refs):
        out_ref[...] = done_ref[m ^ me_ref[0]]


def body(wave_val, wave_con, excite, screening, pair_count, pair_kpoint, pair_partner):
    groups = lax.axis_size("kgrp")
    shards = lax.axis_size("scr")
    slots = pair_kpoint.shape[1]
    nval, mu_dev = wave_val.shape[1:]
    ncon = wave_con.shape[1]
    rows_dev, nexc = excite.shape[1:]
    keep = ncon + nexc * rows_dev // mu_dev
    npb = nval * ncon
    per = LANES // nexc
    parts = nval // per
    split = shards // parts
    vmem = pl.BlockSpec(memory_space=pltpu.VMEM)
    smem = pl.BlockSpec(memory_space=pltpu.SMEM)
    mine_con, mine_val = pl.pallas_call(
        prepare_kernel,
        out_shape=(
            jax.ShapeDtypeStruct((groups, keep, mu_dev), BF16),
            jax.ShapeDtypeStruct((groups, nval, mu_dev), BF16),
        ),
        in_specs=[vmem] * 3,
        out_specs=(vmem, vmem),
    )(wave_con, excite[0].T, wave_val)
    all_con = lax.all_to_all(mine_con, "kgrp", 0, 0, tiled=True)
    all_val = lax.all_to_all(mine_val, "kgrp", 0, 0, tiled=True)
    selected = pl.pallas_call(
        pick_kernel,
        out_shape=jax.ShapeDtypeStruct((2 * slots, keep, mu_dev), BF16),
        in_specs=[smem, smem, vmem],
        out_specs=vmem,
    )(pair_kpoint, pair_partner, all_con)
    gathered = lax.all_gather(selected, "scr", axis=0, tiled=False)
    direct = split == 1 and shards & (shards - 1) == 0
    me = lax.axis_index("scr") if direct else 0
    block = jax.ShapeDtypeStruct((slots, 2, nexc, per * ncon), BF16)
    partial = pl.pallas_call(
        functools.partial(main_kernel, (slots, nval, ncon, nexc)),
        out_shape=(block,) * parts,
        in_specs=[smem, smem, smem, vmem, vmem, vmem],
        out_specs=(vmem,) * parts,
        scratch_shapes=[
            pltpu.VMEM((parts,) + block.shape, BF16),
            pltpu.VMEM((npb, shards * mu_dev), BF16),
            pltpu.VMEM((npb, mu_dev), BF16),
            pltpu.VMEM((npb, mu_dev), BF16),
            pltpu.VMEM((npb // per, npb * per), BF16),
            pltpu.VMEM((npb, LANES), F32),
            pltpu.VMEM((npb * per, LANES), BF16),
        ],
        compiler_params=pltpu.CompilerParams(vmem_limit_bytes=48 * 2**20),
    )(
        pair_kpoint, pair_partner, jnp.full((1,), me, jnp.int32),
        gathered, all_val, screening[0],
    )
    if direct:
        taken = [partial[0]] + [
            lax.ppermute(partial[m], "scr", [(i, i ^ m) for i in range(shards)])
            for m in range(shards - 1, 0, -1)
        ]
    else:
        sent = jnp.stack(partial).reshape(parts, slots, 2, nexc, split, rows_dev)
        sent = sent.transpose(0, 4, 1, 2, 3, 5).reshape(shards, slots, 2, nexc, rows_dev)
        sent = lax.all_to_all(sent, "scr", 0, 0, tiled=True)
        taken = [sent[i] for i in range(shards)]
    live = (jnp.arange(slots, dtype=jnp.int32) < pair_count[0]).astype(F32)
    summed = sum(t.astype(F32) for t in taken) * live[:, None, None, None]
    return (
        summed[None, :, 0].transpose(0, 1, 3, 2),
        summed[None, :, 1].transpose(0, 1, 3, 2),
    )


def solution(mesh):
    return jax.shard_map(
        body,
        mesh=mesh,
        in_specs=(
            P("kgrp", None, "scr"),
            P("kgrp", None, "scr"),
            P("kgrp", "scr", None),
            P("kgrp", None, "scr"),
            P("kgrp"),
            P("kgrp", None),
            P("kgrp", None),
        ),
        out_specs=(P("kgrp", None, "scr", None), P("kgrp", None, "scr", None)),
        check_vma=False,
    )
```

```python
import functools

import jax
import jax.numpy as jnp
from jax import lax
from jax.experimental import pallas as pl
from jax.experimental.pallas import tpu as pltpu
from jax.sharding import PartitionSpec as P

LANES = 128
F32 = jnp.float32
BF16 = jnp.bfloat16


def prepare_kernel(con_ref, exc_ref, val_ref, first_ref, second_ref):
    ncon = con_ref.shape[1]
    rows_dev = exc_ref.shape[1]
    step = con_ref.shape[2] // rows_dev
    exc_rows = exc_ref.shape[0] // step
    packed = jnp.concatenate(
        [exc_ref[i * exc_rows : (i + 1) * exc_rows, :] for i in range(step)], axis=1
    )
    for k in range(first_ref.shape[0]):
        first_ref[k, :ncon, :] = con_ref[0]
        first_ref[k, ncon:, :] = packed
        second_ref[k] = val_ref[0]


def pick_kernel(a_ref, b_ref, all_ref, out_ref):
    slots = a_ref.shape[1]
    for p in range(slots):
        out_ref[p] = all_ref[a_ref[0, p]]
        out_ref[slots + p] = all_ref[b_ref[0, p]]


def nt(a, b):
    return lax.dot_general(a, b, (((1,), (1,)), ((), ())), preferred_element_type=F32)


def pair_products(outer, inner, out_ref, column):
    width = inner.shape[1]
    count = inner.shape[0]
    for i in range(outer.shape[0]):
        out_ref[i * count : (i + 1) * count, pl.ds(column, width)] = (
            outer[i : i + 1, :] * inner
        ).astype(BF16)


def spread_blocks(kernel, out_ref, group):
    block = kernel.shape[0] // group
    tile = out_ref.shape[1] // group
    for i in range(group):
        for q in range(kernel.shape[1] // tile):
            out_ref[q * block : (q + 1) * block, i * tile : (i + 1) * tile] = kernel[
                i * block : (i + 1) * block, q * tile : (q + 1) * tile
            ]


def lay_out(total, parts, nexc):
    flip = total.T
    inner = total.shape[0] // parts
    rows = []
    for s in range(parts):
        rows.append(
            jnp.concatenate(
                [
                    flip[i * nexc : (i + 1) * nexc, s * inner : (s + 1) * inner]
                    for i in range(total.shape[1] // nexc)
                ],
                axis=1,
            )
        )
    return jnp.concatenate(rows, axis=0)


def screen_kernel(sizes, ids_ref, weights_ref, *rest):
    slots, ncon, shards = sizes
    gath_refs, (out_ref, rho_ref) = rest[:shards], rest[shards:]
    mu_dev = weights_ref.shape[1]
    for p in range(slots):
        for m, gath_ref in enumerate(gath_refs):
            pair_products(
                gath_ref[slots + p, :ncon, :].astype(F32),
                gath_ref[p, :ncon, :].astype(F32),
                rho_ref, pl.multiple_of(ids_ref[m] * mu_dev, mu_dev),
            )
        out_ref[p] = jnp.dot(
            rho_ref[...], weights_ref[...], preferred_element_type=F32
        ).astype(BF16)


def main_kernel(
    sizes, a_ref, b_ref, ids_ref, all_ref, screened_ref, *rest
):
    shards, direct = sizes[4:]
    sizes = sizes[:4]
    gath_refs, rest = rest[:shards], rest[shards:]
    *out_refs, done_ref, vals_ref, spread_ref, vec_ref, diag_ref = rest
    slots, nval, ncon, nexc = sizes
    mu_dev = screened_ref.shape[2]
    rows_dev = nval * ncon // shards
    per = LANES // nexc
    parts = done_ref.shape[0]
    lane = lax.broadcasted_iota(jnp.int32, (per * nval, LANES), 1)
    row = lax.broadcasted_iota(jnp.int32, (per * nval, LANES), 0)
    mask = (row // nval == lane // nexc).astype(BF16)
    e_row = lax.broadcasted_iota(jnp.int32, (nexc, LANES), 0)
    e_lane = lax.broadcasted_iota(jnp.int32, (nexc, LANES), 1)
    repeat = (e_lane % nexc == e_row).astype(BF16)
    wide = ncon * per
    src = lax.broadcasted_iota(jnp.int32, (wide, wide), 0)
    dst = lax.broadcasted_iota(jnp.int32, (wide, wide), 1)
    few = nval // parts
    outer = ncon // per
    moved = (src % few) * ncon + (src // few) % outer * per + src // (few * outer)
    order = (moved == dst).astype(BF16)
    for p in range(slots):
        pair_products(
            all_ref[a_ref[0, p]].astype(F32), all_ref[b_ref[0, p]].astype(F32), vals_ref, 0
        )
        for way in range(2):
            who = slots + p if way == 0 else p
            for gath_ref, m in zip(gath_refs, range(shards)):
                part = gath_ref[who, ncon:, :]
                at = pl.multiple_of(ids_ref[m] * rows_dev, rows_dev)
                flip = jnp.concatenate(
                    [part[:, i * rows_dev : (i + 1) * rows_dev] for i in range(mu_dev // rows_dev)], axis=0
                )
                vec_ref[pl.ds(at, rows_dev), :] = lax.dot_general(
                    flip, repeat, (((0,), (0,)), ((), ())), preferred_element_type=F32
                )
            if way == 0:
                kernel = nt(screened_ref[p], vals_ref[...]).astype(BF16)
                count, length = ncon, nval
            else:
                kernel = nt(vals_ref[...], screened_ref[p]).astype(BF16)
                count, length = nval, ncon
            spread_blocks(kernel, spread_ref, count)
            for i in range(count):
                if way == 0:
                    vec = vec_ref[pl.ds(i, length, stride=count), :]
                else:
                    vec = vec_ref[i * length : (i + 1) * length, :]
                vec = vec.astype(BF16)
                tile = per * length
                diag_ref[i * tile : (i + 1) * tile, :] = (
                    jnp.concatenate([vec] * per, axis=0) * mask
                )
            total = jnp.dot(spread_ref[...], diag_ref[...], preferred_element_type=F32)
            if way == 0:
                done = lay_out(total, parts, nexc)
            else:
                total = total.reshape(outer, parts, few, LANES)
                total = jnp.concatenate(
                    [total[q, s] for s in range(parts) for q in range(outer)], axis=0
                )
                done = jnp.dot(
                    lay_out(total, parts, nexc).astype(BF16), order, preferred_element_type=F32
                )
            done = done.astype(BF16)
            for s in range(parts):
                done_ref[s, p, way] = done[s * nexc : (s + 1) * nexc, :]
    for m, out_ref in enumerate(out_refs):
        out_ref[...] = done_ref[ids_ref[m] if direct else m]


def body(wave_val, wave_con, excite, screening, pair_count, pair_kpoint, pair_partner):
    groups = lax.axis_size("kgrp")
    shards = lax.axis_size("scr")
    slots = pair_kpoint.shape[1]
    nval, mu_dev = wave_val.shape[1:]
    ncon = wave_con.shape[1]
    rows_dev, nexc = excite.shape[1:]
    keep = ncon + nexc * rows_dev // mu_dev
    npb = nval * ncon
    per = LANES // nexc
    parts = nval // per
    split = shards // parts
    vmem = pl.BlockSpec(memory_space=pltpu.VMEM)
    smem = pl.BlockSpec(memory_space=pltpu.SMEM)
    mine_con, mine_val = pl.pallas_call(
        prepare_kernel,
        out_shape=(
            jax.ShapeDtypeStruct((groups, keep, mu_dev), BF16),
            jax.ShapeDtypeStruct((groups, nval, mu_dev), BF16),
        ),
        in_specs=[vmem] * 3,
        out_specs=(vmem, vmem),
        cost_estimate=pl.CostEstimate(flops=0, transcendentals=0, bytes_accessed=6 * 2**20),
    )(wave_con, excite[0].T, wave_val)
    all_con = lax.all_to_all(mine_con, "kgrp", 0, 0, tiled=True)
    all_val = lax.all_to_all(mine_val, "kgrp", 0, 0, tiled=True)
    selected = pl.pallas_call(
        pick_kernel,
        out_shape=jax.ShapeDtypeStruct((2 * slots, keep, mu_dev), BF16),
        in_specs=[smem, smem, vmem],
        out_specs=vmem,
        compiler_params=pltpu.CompilerParams(vmem_limit_bytes=8 * 2**20),
    )(pair_kpoint, pair_partner, all_con)
    direct = split == 1 and shards & (shards - 1) == 0
    if direct:
        ids = lax.axis_index("scr") ^ jnp.arange(shards, dtype=jnp.int32)
        found = {0: selected}
        step = shards
        while step > 1:
            step //= 2
            for m in sorted(found):
                found[m | step] = lax.ppermute(
                    found[m], "scr", [(i, i ^ step) for i in range(shards)]
                )
        gathered = [found[m] for m in range(shards)]
    else:
        ids = jnp.arange(shards, dtype=jnp.int32)
        gathered = lax.all_gather(selected, "scr", axis=0, tiled=False)
        gathered = [gathered[m] for m in range(shards)]
    block = jax.ShapeDtypeStruct((slots, 2, nexc, per * ncon), BF16)
    limit = pltpu.CompilerParams(vmem_limit_bytes=24 * 2**20)
    screened = pl.pallas_call(
        functools.partial(screen_kernel, (slots, ncon, shards)),
        out_shape=jax.ShapeDtypeStruct((slots, npb, mu_dev), BF16),
        in_specs=[smem] + [vmem] * (1 + shards),
        out_specs=vmem,
        scratch_shapes=[pltpu.VMEM((npb, shards * mu_dev), BF16)],
        compiler_params=limit,
    )(ids, screening[0], *gathered)
    partial = pl.pallas_call(
        functools.partial(main_kernel, (slots, nval, ncon, nexc, shards, direct)),
        out_shape=(block,) * parts,
        in_specs=[smem] * 3 + [vmem] * (2 + shards),
        out_specs=(vmem,) * parts,
        scratch_shapes=[
            pltpu.VMEM((parts,) + block.shape, BF16),
            pltpu.VMEM((npb, mu_dev), BF16),
            pltpu.VMEM((npb // per, npb * per), BF16),
            pltpu.VMEM((npb, LANES), F32),
            pltpu.VMEM((npb * per, LANES), BF16),
        ],
        compiler_params=limit,
    )(pair_kpoint, pair_partner, ids, all_val, screened, *gathered)
    if direct:
        taken = [partial[0]] + [
            lax.ppermute(partial[m], "scr", [(i, i ^ m) for i in range(shards)])
            for m in range(shards - 1, 0, -1)
        ]
    else:
        sent = jnp.stack(partial).reshape(parts, slots, 2, nexc, split, rows_dev)
        sent = sent.transpose(0, 4, 1, 2, 3, 5).reshape(shards, slots, 2, nexc, rows_dev)
        sent = lax.all_to_all(sent, "scr", 0, 0, tiled=True)
        taken = [sent[i] for i in range(shards)]
    live = (jnp.arange(slots, dtype=jnp.int32) < pair_count[0]).astype(F32)
    summed = sum(t.astype(F32) for t in taken) * live[:, None, None, None]
    return (
        summed[None, :, 0].transpose(0, 1, 3, 2),
        summed[None, :, 1].transpose(0, 1, 3, 2),
    )


def solution(mesh):
    return jax.shard_map(
        body,
        mesh=mesh,
        in_specs=(
            P("kgrp", None, "scr"),
            P("kgrp", None, "scr"),
            P("kgrp", "scr", None),
            P("kgrp", None, "scr"),
            P("kgrp"),
            P("kgrp", None),
            P("kgrp", None),
        ),
        out_specs=(P("kgrp", None, "scr", None), P("kgrp", None, "scr", None)),
        check_vma=False,
    )
```

```python
import functools

import jax
import jax.numpy as jnp
from jax import lax
from jax.experimental import pallas as pl
from jax.experimental.pallas import tpu as pltpu
from jax.sharding import PartitionSpec as P

LANES = 128
F32 = jnp.float32
BF16 = jnp.bfloat16


def prepare_kernel(
    a_ref, b_ref, con_ref, exc_ref, val_ref, first_ref, second_ref, roles_ref
):
    slots = a_ref.shape[1]
    for p in range(slots):
        roles_ref[p] = a_ref[0, p]
        roles_ref[slots + p] = b_ref[0, p]
    ncon = con_ref.shape[1]
    rows_dev = exc_ref.shape[1]
    step = con_ref.shape[2] // rows_dev
    exc_rows = exc_ref.shape[0] // step
    packed = jnp.concatenate(
        [exc_ref[i * exc_rows : (i + 1) * exc_rows, :] for i in range(step)], axis=1
    )
    for k in range(first_ref.shape[0]):
        first_ref[k, :ncon, :] = con_ref[0]
        first_ref[k, ncon:, :] = packed
        second_ref[k] = val_ref[0]


def pick_kernel(roles_ref, all_ref, out_ref):
    for i in range(out_ref.shape[0]):
        out_ref[i] = all_ref[roles_ref[i]]


def nt(a, b):
    return lax.dot_general(a, b, (((1,), (1,)), ((), ())), preferred_element_type=F32)


def pair_products(outer, inner, out_ref, column):
    width = inner.shape[1]
    count = inner.shape[0]
    for i in range(outer.shape[0]):
        out_ref[i * count : (i + 1) * count, pl.ds(column, width)] = (
            outer[i : i + 1, :] * inner
        ).astype(BF16)


def spread_blocks(kernel, out_ref, group):
    block = kernel.shape[0] // group
    tile = out_ref.shape[1] // group
    for i in range(group):
        for q in range(kernel.shape[1] // tile):
            out_ref[q * block : (q + 1) * block, i * tile : (i + 1) * tile] = kernel[
                i * block : (i + 1) * block, q * tile : (q + 1) * tile
            ]


def lay_out(total, parts, nexc):
    flip = total.T
    inner = total.shape[0] // parts
    rows = []
    for s in range(parts):
        rows.append(
            jnp.concatenate(
                [
                    flip[i * nexc : (i + 1) * nexc, s * inner : (s + 1) * inner]
                    for i in range(total.shape[1] // nexc)
                ],
                axis=1,
            )
        )
    return jnp.concatenate(rows, axis=0)


def screen_kernel(sizes, ids_ref, weights_ref, *rest):
    slots, ncon, shards = sizes
    gath_refs, (out_ref, rho_ref) = rest[:shards], rest[shards:]
    mu_dev = weights_ref.shape[1]
    for p in range(slots):
        for m, gath_ref in enumerate(gath_refs):
            pair_products(
                gath_ref[slots + p, :ncon, :].astype(F32),
                gath_ref[p, :ncon, :].astype(F32),
                rho_ref, pl.multiple_of(ids_ref[m] * mu_dev, mu_dev),
            )
        out_ref[p] = jnp.dot(
            rho_ref[...], weights_ref[...], preferred_element_type=F32
        ).astype(BF16)


def main_kernel(
    sizes, roles_ref, ids_ref, all_ref, screened_ref, *rest
):
    shards, direct = sizes[4:]
    sizes = sizes[:4]
    gath_refs, rest = rest[:shards], rest[shards:]
    *out_refs, done_ref, vals_ref, spread_ref, vec_ref, diag_ref = rest
    slots, nval, ncon, nexc = sizes
    mu_dev = screened_ref.shape[2]
    rows_dev = nval * ncon // shards
    per = LANES // nexc
    parts = done_ref.shape[0]
    lane = lax.broadcasted_iota(jnp.int32, (per * nval, LANES), 1)
    row = lax.broadcasted_iota(jnp.int32, (per * nval, LANES), 0)
    mask = (row // nval == lane // nexc).astype(BF16)
    e_row = lax.broadcasted_iota(jnp.int32, (nexc, LANES), 0)
    e_lane = lax.broadcasted_iota(jnp.int32, (nexc, LANES), 1)
    repeat = (e_lane % nexc == e_row).astype(BF16)
    wide = ncon * per
    src = lax.broadcasted_iota(jnp.int32, (wide, wide), 0)
    dst = lax.broadcasted_iota(jnp.int32, (wide, wide), 1)
    few = nval // parts
    outer = ncon // per
    moved = (src % few) * ncon + (src // few) % outer * per + src // (few * outer)
    order = (moved == dst).astype(BF16)
    for p in range(slots):
        pair_products(
            all_ref[roles_ref[p]].astype(F32), all_ref[roles_ref[slots + p]].astype(F32), vals_ref, 0
        )
        for way in range(2):
            who = slots + p if way == 0 else p
            for gath_ref, m in zip(gath_refs, range(shards)):
                part = gath_ref[who, ncon:, :]
                at = pl.multiple_of(ids_ref[m] * rows_dev, rows_dev)
                flip = jnp.concatenate(
                    [part[:, i * rows_dev : (i + 1) * rows_dev] for i in range(mu_dev // rows_dev)], axis=0
                )
                vec_ref[pl.ds(at, rows_dev), :] = lax.dot_general(
                    flip, repeat, (((0,), (0,)), ((), ())), preferred_element_type=F32
                )
            if way == 0:
                kernel = nt(screened_ref[p], vals_ref[...]).astype(BF16)
                count, length = ncon, nval
            else:
                kernel = nt(vals_ref[...], screened_ref[p]).astype(BF16)
                count, length = nval, ncon
            spread_blocks(kernel, spread_ref, count)
            for i in range(count):
                if way == 0:
                    vec = vec_ref[pl.ds(i, length, stride=count), :]
                else:
                    vec = vec_ref[i * length : (i + 1) * length, :]
                vec = vec.astype(BF16)
                tile = per * length
                diag_ref[i * tile : (i + 1) * tile, :] = (
                    jnp.concatenate([vec] * per, axis=0) * mask
                )
            total = jnp.dot(spread_ref[...], diag_ref[...], preferred_element_type=F32)
            if way == 0:
                done = lay_out(total, parts, nexc)
            else:
                total = total.reshape(outer, parts, few, LANES)
                total = jnp.concatenate(
                    [total[q, s] for s in range(parts) for q in range(outer)], axis=0
                )
                done = jnp.dot(
                    lay_out(total, parts, nexc).astype(BF16), order, preferred_element_type=F32
                )
            done = done.astype(BF16)
            for s in range(parts):
                done_ref[s, p, way] = done[s * nexc : (s + 1) * nexc, :]
    for m, out_ref in enumerate(out_refs):
        out_ref[...] = done_ref[ids_ref[m] if direct else m]


def body(wave_val, wave_con, excite, screening, pair_count, pair_kpoint, pair_partner):
    groups = lax.axis_size("kgrp")
    shards = lax.axis_size("scr")
    slots = pair_kpoint.shape[1]
    nval, mu_dev = wave_val.shape[1:]
    ncon = wave_con.shape[1]
    rows_dev, nexc = excite.shape[1:]
    keep = ncon + nexc * rows_dev // mu_dev
    npb = nval * ncon
    per = LANES // nexc
    parts = nval // per
    split = shards // parts
    vmem = pl.BlockSpec(memory_space=pltpu.VMEM)
    smem = pl.BlockSpec(memory_space=pltpu.SMEM)
    mine_con, mine_val, roles = pl.pallas_call(
        prepare_kernel,
        out_shape=(
            jax.ShapeDtypeStruct((groups, keep, mu_dev), BF16),
            jax.ShapeDtypeStruct((groups, nval, mu_dev), BF16),
            jax.ShapeDtypeStruct((2 * slots,), jnp.int32),
        ),
        in_specs=[smem] * 2 + [vmem] * 3,
        out_specs=(vmem, vmem, smem),
        cost_estimate=pl.CostEstimate(flops=0, transcendentals=0, bytes_accessed=6 * 2**20),
    )(pair_kpoint, pair_partner, wave_con, excite[0].T, wave_val)
    all_con = lax.all_to_all(mine_con, "kgrp", 0, 0, tiled=True)
    all_val = lax.all_to_all(mine_val, "kgrp", 0, 0, tiled=True)
    selected = pl.pallas_call(
        pick_kernel,
        out_shape=jax.ShapeDtypeStruct((2 * slots, keep, mu_dev), BF16),
        in_specs=[smem, vmem],
        out_specs=vmem,
        compiler_params=pltpu.CompilerParams(vmem_limit_bytes=8 * 2**20),
    )(roles, all_con)
    direct = split == 1 and shards & (shards - 1) == 0
    if direct:
        ids = lax.axis_index("scr") ^ jnp.arange(shards, dtype=jnp.int32)
        found = {0: selected}
        step = shards
        while step > 1:
            step //= 2
            for m in sorted(found):
                found[m | step] = lax.ppermute(
                    found[m], "scr", [(i, i ^ step) for i in range(shards)]
                )
        gathered = [found[m] for m in range(shards)]
    else:
        ids = jnp.arange(shards, dtype=jnp.int32)
        gathered = lax.all_gather(selected, "scr", axis=0, tiled=False)
        gathered = [gathered[m] for m in range(shards)]
    block = jax.ShapeDtypeStruct((slots, 2, nexc, per * ncon), BF16)
    limit = pltpu.CompilerParams(vmem_limit_bytes=24 * 2**20)
    screened = pl.pallas_call(
        functools.partial(screen_kernel, (slots, ncon, shards)),
        out_shape=jax.ShapeDtypeStruct((slots, npb, mu_dev), BF16),
        in_specs=[smem] + [vmem] * (1 + shards),
        out_specs=vmem,
        scratch_shapes=[pltpu.VMEM((npb, shards * mu_dev), BF16)],
        compiler_params=limit,
    )(ids, screening[0], *gathered)
    partial = pl.pallas_call(
        functools.partial(main_kernel, (slots, nval, ncon, nexc, shards, direct)),
        out_shape=(block,) * parts,
        in_specs=[smem] * 2 + [vmem] * (2 + shards),
        out_specs=(vmem,) * parts,
        scratch_shapes=[
            pltpu.VMEM((parts,) + block.shape, BF16),
            pltpu.VMEM((npb, mu_dev), BF16),
            pltpu.VMEM((npb // per, npb * per), BF16),
            pltpu.VMEM((npb, LANES), F32),
            pltpu.VMEM((npb * per, LANES), BF16),
        ],
        compiler_params=limit,
    )(roles, ids, all_val, screened, *gathered)
    if direct:
        taken = [partial[0]]
        for m in range(shards - 1, 0, -1):
            taken.append(
                lax.ppermute(partial[m], "scr", [(i, i ^ m) for i in range(shards)])
            )
    else:
        sent = jnp.stack(partial).reshape(parts, slots, 2, nexc, split, rows_dev)
        sent = sent.transpose(0, 4, 1, 2, 3, 5).reshape(shards, slots, 2, nexc, rows_dev)
        sent = lax.all_to_all(sent, "scr", 0, 0, tiled=True)
        taken = [sent[i] for i in range(shards)]
    live = (jnp.arange(slots, dtype=jnp.int32) < pair_count[0]).astype(F32)
    summed = sum(t.astype(F32) for t in taken) * live[:, None, None, None]
    return (
        summed[None, :, 0].transpose(0, 1, 3, 2),
        summed[None, :, 1].transpose(0, 1, 3, 2),
    )


def solution(mesh):
    return jax.shard_map(
        body,
        mesh=mesh,
        in_specs=(
            P("kgrp", None, "scr"),
            P("kgrp", None, "scr"),
            P("kgrp", "scr", None),
            P("kgrp", None, "scr"),
            P("kgrp"),
            P("kgrp", None),
            P("kgrp", None),
        ),
        out_specs=(P("kgrp", None, "scr", None), P("kgrp", None, "scr", None)),
        check_vma=False,
    )
```
